32 devices in a mesh: pairs: 2 (over y), gx: 4 (over z), gy: 2 (over x), gz: 2 (over core).
Axes of the slice: x: 2, y: 2, z: 4, core: 2. Of those that a mesh axis runs over, the one named last changes fastest.
Arguments:
- fine_start: float32 [64, 128, 512], P(('pairs', 'gx'), 'gy', 'gz'), parts along dimension 0, may hold values from -1 to 1
- increments: float32 [2, 64, 128, 512], P(None, ('pairs', 'gx'), 'gy', 'gz'), parts along dimension 1, may hold values from -5 to 5
- coarse_start: float32 [32, 64, 256], P(('pairs', 'gx')), parts along dimension 0, may hold values from -1 to 1
Outputs:
- fine_final: float32 [64, 128, 512], P(('pairs', 'gx'), 'gy', 'gz'), parts along dimension 0
- coarse_final: float32 [32, 64, 256], P(('pairs', 'gx')), parts along dimension 0
The draws below stay inside these ranges and needn't reach their ends.
There are 2 independent parts, one for each index of `pairs`. The reference program is written for one: setup_inputs(seed, part) draws one part's arguments, and reference() takes and returns one part's arrays. A program takes and returns all parts, laid end to end along the dimension named above; each array names one. Nothing has to cross between parts.
All inputs are finite; a program needn't handle non-finite values.
Results may differ from the reference program's by a relative error of at most 0.00002.
Values sent between devices are 32-bit elements; how exact they have to be, the bound alone decides.
No kernel may reach another device: no remote copies, remote signals or barrier semaphores. Data moves between devices by JAX's collectives and lax.ppermute only.
A program may use at most 128 MiB of HBM per device.

```python
import jax
import jax.numpy as jnp

STEPS = 2
SWEEPS = 2
NX = 32
NY = 128
NZ = 512


def draw_increments(key, part):
    extent = (STEPS, NX, NY, NZ)
    values = jnp.clip(jax.random.normal(key, extent, jnp.float32), -5.0, 5.0)
    return values


def shard_levels(stream_key, shape, shards, least, largest):
    def one(axis_at, blocks):
        steps = jax.random.uniform(jax.random.fold_in(jax.random.fold_in(stream_key, 6), axis_at), (blocks,), jnp.float32, least / len(shards), largest / len(shards))
        return jnp.repeat(jnp.exp(steps), shape[axis_at] // blocks).reshape((-1,) + (1,) * (len(shape) - axis_at - 1))

    gain = one(*shards[0])
    for cut in shards[1:]:
        gain = gain * one(*cut)
    return gain


def setup_inputs(seed: int = 0, part: int = 0) -> dict:
    seeds = jax.random.split(jax.random.key(seed), 4)
    own_keys = jax.random.split(jax.random.fold_in(seeds[3], part), 4)
    fine_start = jnp.clip(jax.random.uniform(own_keys[0], (NX, NY, NZ), jnp.float32, -1.0, 1.0) * shard_levels(own_keys[0], (NX, NY, NZ), ((0, 4), (1, 2), (2, 2)), -0.4, 0.0), -1.0, 1.0)
    increments = draw_increments(jax.random.fold_in(jax.random.fold_in(seeds[3], part), 71), part)
    coarse_start = jnp.clip(jax.random.uniform(own_keys[2], (NX // 2, NY // 2, NZ // 2), jnp.float32, -1.0, 1.0) * shard_levels(own_keys[2], (NX // 2, NY // 2, NZ // 2), ((0, 4),), -0.4, 0.0), -1.0, 1.0)
    return dict(fine_start=fine_start, increments=increments, coarse_start=coarse_start)


noise_scale = 0.3
fine_step = 0.2
coarse_step = 0.4
fine_coupling = 1.0
coarse_coupling = 0.5


def neighbours(padded):
    beside = padded[2:, 1:-1, 1:-1] + padded[:-2, 1:-1, 1:-1]
    beside = beside + padded[1:-1, 2:, 1:-1] + padded[1:-1, :-2, 1:-1]
    beside = beside + padded[1:-1, 1:-1, 2:] + padded[1:-1, 1:-1, :-2]
    return beside


def advance(state, forcing, step_size, coupling):
    source = state + step_size * (state - state * state * state) + noise_scale * forcing
    fields = source
    for sweep_index in range(SWEEPS):
        padded = jnp.pad(fields, 1, mode="wrap")
        fields = (source + coupling * neighbours(padded)) / (1.0 + 6.0 * coupling)
    return fields


def reference(fine_start, increments, coarse_start):
    state = fine_start
    for step_index in range(STEPS):
        state = advance(state, increments[step_index], fine_step, fine_coupling)
    summed = jnp.sum(increments, axis=0)
    coarse_noise = 0.125 * summed.reshape(NX // 2, 2, NY // 2, 2, NZ // 2, 2).sum(axis=(1, 3, 5))
    coarse_final = advance(coarse_start, coarse_noise, coarse_step, coarse_coupling)
    return state, coarse_final
```

```python
import jax
import jax.numpy as jnp
from jax import lax
from jax.sharding import PartitionSpec as P

STEPS = 2
SWEEPS = 2


noise_scale = 0.3
fine_step = 0.2
coarse_step = 0.4
fine_coupling = 1.0
coarse_coupling = 0.5


def with_halo(value, sides, width):
    for axis, dim in sides:
        count, length = (lax.axis_size(axis), value.shape[dim])
        up = [(i, (i + 1) % count) for i in range(count)]
        down = [(j, i) for i, j in up]
        last = lax.slice_in_dim(value, length - width, length, axis=dim)
        first = lax.slice_in_dim(value, 0, width, axis=dim)
        before = lax.ppermute(last, axis, up)
        after = lax.ppermute(first, axis, down)
        value = jnp.concatenate([before, value, after], axis=dim)
    return value


def neighbours(padded):
    beside = padded[2:, 1:-1, 1:-1] + padded[:-2, 1:-1, 1:-1]
    beside = beside + padded[1:-1, 2:, 1:-1] + padded[1:-1, :-2, 1:-1]
    beside = beside + padded[1:-1, 1:-1, 2:] + padded[1:-1, 1:-1, :-2]
    return beside


def trimmed_box(source, margin):
    return source[
        margin : source.shape[0] - margin,
        margin : source.shape[1] - margin,
        margin : source.shape[2] - margin,
    ]


def reaction(state, forcing, step_size):
    return state + step_size * (state - state * state * state) + noise_scale * forcing


def relaxed(source, coupling, extend):
    padded = extend(source, SWEEPS)
    fields = padded
    for sweep_index in range(SWEEPS):
        fields = (trimmed_box(padded, sweep_index + 1) + coupling * neighbours(fields)) / (
            1.0 + 6.0 * coupling
        )
    return fields


def fine_halo(source, width):
    return with_halo(source, (("gx", 0), ("gy", 1), ("gz", 2)), width)


def slab_halo(source, width):
    extended = with_halo(source, (("gx", 0),), width)
    return jnp.pad(extended, ((0, 0), (width, width), (width, width)), mode="wrap")


def assemble(stacked):
    count_y = lax.axis_size("gy")
    count_z = lax.axis_size("gz")
    depth_x, width_y, width_z = (stacked.shape[1], stacked.shape[2], stacked.shape[3])
    blocks = stacked.reshape(count_y, count_z, depth_x, width_y, width_z)
    return blocks.transpose(2, 0, 3, 1, 4).reshape(depth_x, count_y * width_y, count_z * width_z)


def pair_sum(length):
    fine = lax.broadcasted_iota(jnp.int32, (length, length // 2), 0)
    coarse = lax.broadcasted_iota(jnp.int32, (length, length // 2), 1)
    return (fine // 2 == coarse).astype(jnp.float32)


def body(fine_start, increments, coarse_start):
    state = fine_start
    for step_index in range(STEPS):
        state = relaxed(
            reaction(state, increments[step_index], fine_step), fine_coupling, fine_halo
        )
    depth_x, width_y, width_z = increments.shape[1:]
    layers = increments.reshape(STEPS, depth_x // 2, 2, width_y, width_z).sum(axis=(0, 2))
    rows = lax.dot_general(
        layers.reshape(-1, width_z), pair_sum(width_z), (((1,), (0,)), ((), ())), precision="highest"
    ).reshape(depth_x // 2, width_y, width_z // 2)
    partial_value = 0.125 * jnp.einsum("ab,xbz->xaz", pair_sum(width_y).T, rows, precision="highest")
    slab_noise = assemble(lax.all_gather(partial_value[None], ("gy", "gz"), axis=0, tiled=True))
    coarse_final = relaxed(
        reaction(coarse_start, slab_noise, coarse_step), coarse_coupling, slab_halo
    )
    return (state, coarse_final)


def solution(mesh):
    return jax.shard_map(
        body,
        mesh=mesh,
        in_specs=(
            P(("pairs", "gx"), "gy", "gz"),
            P(None, ("pairs", "gx"), "gy", "gz"),
            P(("pairs", "gx"), None, None),
        ),
        out_specs=(P(("pairs", "gx"), "gy", "gz"), P(("pairs", "gx"), None, None)),
        check_vma=False,
    )
```

```python
import jax
import jax.numpy as jnp
from jax import lax
from jax.experimental import pallas as pl
from jax.experimental.pallas import tpu as pltpu
from jax.sharding import PartitionSpec as P


STEPS = 2
SWEEPS = 2


noise_scale = 0.3
fine_step = 0.2
coarse_step = 0.4
fine_coupling = 1.0
coarse_coupling = 0.5


def with_halo(value, sides, width):
    for axis, dim in sides:
        count, length = (lax.axis_size(axis), value.shape[dim])
        up = [(i, (i + 1) % count) for i in range(count)]
        down = [(j, i) for i, j in up]
        last = lax.slice_in_dim(value, length - width, length, axis=dim)
        first = lax.slice_in_dim(value, 0, width, axis=dim)
        before = lax.ppermute(last, axis, up)
        after = lax.ppermute(first, axis, down)
        value = jnp.concatenate([before, value, after], axis=dim)
    return value


def neighbours(padded):
    beside = padded[2:, 1:-1, 1:-1] + padded[:-2, 1:-1, 1:-1]
    beside = beside + padded[1:-1, 2:, 1:-1] + padded[1:-1, :-2, 1:-1]
    beside = beside + padded[1:-1, 1:-1, 2:] + padded[1:-1, 1:-1, :-2]
    return beside


def trimmed_box(source, margin):
    return source[
        margin : source.shape[0] - margin,
        margin : source.shape[1] - margin,
        margin : source.shape[2] - margin,
    ]


def reaction(state, forcing, step_size):
    return state + step_size * (state - state * state * state) + noise_scale * forcing


def relaxed(source, coupling, extend):
    padded = extend(source, SWEEPS)
    fields = padded
    for sweep_index in range(SWEEPS):
        fields = (trimmed_box(padded, sweep_index + 1) + coupling * neighbours(fields)) / (
            1.0 + 6.0 * coupling
        )
    return fields


def fine_halo(source, width):
    return with_halo(source, (("gx", 0), ("gy", 1), ("gz", 2)), width)


def slab_halo(source, width):
    extended = with_halo(source, (("gx", 0),), width)
    return jnp.pad(extended, ((0, 0), (width, width), (width, width)), mode="wrap")


def assemble(stacked):
    count_y = lax.axis_size("gy")
    count_z = lax.axis_size("gz")
    depth_x, width_y, width_z = (stacked.shape[1], stacked.shape[2], stacked.shape[3])
    blocks = stacked.reshape(count_y, count_z, depth_x, width_y, width_z)
    return blocks.transpose(2, 0, 3, 1, 4).reshape(depth_x, count_y * width_y, count_z * width_z)


def pair_sum(length):
    fine = lax.broadcasted_iota(jnp.int32, (length, length // 2), 0)
    coarse = lax.broadcasted_iota(jnp.int32, (length, length // 2), 1)
    return (fine // 2 == coarse).astype(jnp.float32)


def staged(fine_start, increments, coarse_start):
    state = fine_start
    for step_index in range(STEPS):
        state = relaxed(
            reaction(state, increments[step_index], fine_step), fine_coupling, fine_halo
        )
    depth_x, width_y, width_z = increments.shape[1:]
    layers = increments.reshape(STEPS, depth_x // 2, 2, width_y, width_z).sum(axis=(0, 2))
    rows = lax.dot_general(
        layers.reshape(-1, width_z), pair_sum(width_z), (((1,), (0,)), ((), ())), precision="highest"
    ).reshape(depth_x // 2, width_y, width_z // 2)
    partial_value = 0.125 * jnp.einsum("ab,xbz->xaz", pair_sum(width_y).T, rows, precision="highest")
    slab_noise = assemble(lax.all_gather(partial_value[None], ("gy", "gz"), axis=0, tiled=True))
    coarse_final = relaxed(
        reaction(coarse_start, slab_noise, coarse_step), coarse_coupling, slab_halo
    )
    return (state, coarse_final)


LANES = 128
ROWS = 8
REACH = STEPS * SWEEPS

TOP = ROWS
CELLS = 2 * ROWS
CHUNK = 2 * ROWS


def call(kernel, outs, args, scratch=(), specs=None, flops=2000000):
    return pl.pallas_call(
        kernel,
        out_shape=[jax.ShapeDtypeStruct(shape, jnp.float32) for shape in outs],
        in_specs=specs or [pl.BlockSpec(memory_space=pltpu.VMEM)] * len(args),
        out_specs=[pl.BlockSpec(memory_space=pltpu.VMEM)] * len(outs),
        scratch_shapes=list(scratch),
        compiler_params=pltpu.CompilerParams(vmem_limit_bytes=16 * 1024 * 1024),
        cost_estimate=pl.CostEstimate(flops=flops, bytes_accessed=1000000, transcendentals=0),
    )(*args)


def edge_rows(value):
    length = value.shape[1]
    row = lax.broadcasted_iota(jnp.int32, (value.shape[0], ROWS, value.shape[2]), 1)
    return jnp.where(row < ROWS // 2, value[:, :ROWS], value[:, length - ROWS :])


def edge_lanes(value):
    length = value.shape[2]
    lane = lax.broadcasted_iota(jnp.int32, value.shape[:2] + (LANES,), 2)
    return jnp.where(lane < LANES // 2, value[:, :, :LANES], value[:, :, length - LANES :])


def upward():
    return lax.axis_index("gx") % 2 == 0


def pack_rows(quarter, target, first):
    for tile in range(quarter.shape[0] * quarter.shape[1] // (2 * ROWS)):
        plane, at = divmod(tile * 2 * ROWS, quarter.shape[1])
        rows = slice(first + tile * ROWS, first + (tile + 1) * ROWS)
        target[rows, :LANES] = quarter[plane, at : at + ROWS]
        target[rows, LANES:] = quarter[plane, at + ROWS : at + 2 * ROWS]


def unpack_rows(source, first, planes, height):
    parts = []
    for tile in range(planes * height // (2 * ROWS)):
        rows = slice(first + tile * ROWS, first + (tile + 1) * ROWS)
        parts += [source[rows, :LANES], source[rows, LANES:]]
    return jnp.concatenate(parts, axis=0).reshape(planes, height, LANES)


def open_kernel(own, inc, coarse, band, side, corner, quarter, pairs):
    depth, width, length = own.shape
    half_y, half_z = width // 2, length // 2
    value, later = own[...], inc[1]
    band[:, :ROWS] = edge_rows(value)
    band[:, ROWS : 2 * ROWS] = edge_rows(later)
    side[:, :width] = edge_lanes(value)
    side[:, width:] = edge_lanes(later)
    corner[...] = edge_lanes(band[...])
    layers = (inc[0] + later).reshape(depth // 2, 2, width, length)
    layers = layers[:, 0] + layers[:, 1]
    parts = []
    for tile in range(length // LANES):
        pairs[tile] = layers[:, :, tile * LANES : (tile + 1) * LANES]
        parts.append(
            pairs[tile, :, pl.ds(0, half_y, 2), :] + pairs[tile, :, pl.ds(1, half_y, 2), :]
        )
    rows = jnp.concatenate(parts, axis=2)
    summed = jnp.dot(
        rows.reshape(-1, length),
        pair_sum(length),
        precision=lax.Precision.HIGHEST,
        preferred_element_type=jnp.float32,
    ).reshape(depth // 2, half_y, half_z)
    at_y = pl.multiple_of(lax.axis_index("gy") * half_y, half_y)
    at_z = pl.multiple_of(lax.axis_index("gz") * half_z, half_z)
    start = coarse[:, pl.ds(at_y, half_y), pl.ds(at_z, half_z)]
    quarter[...] = reaction(start, 0.125 * summed, coarse_step)


def put_plane(target, cells, band, side, corner):
    width = cells.shape[0]
    for tile, part in enumerate((slice(0, LANES), slice(LANES, 2 * LANES))):
        target[tile, TOP:CELLS] = band[:, part]
        target[tile, CELLS : CELLS + width] = cells[:, part]
        target[tile, CELLS + width : CELLS + width + ROWS] = band[:, part]
    target[2, TOP:CELLS] = corner
    target[2, CELLS : CELLS + width] = side
    target[2, CELLS + width : CELLS + width + ROWS] = corner


def spread_kernel(own, inc, quarter, band, side, corner, whole, later, first, second):
    depth, width, _ = own.shape
    lane = lax.broadcasted_iota(jnp.int32, (ROWS, LANES), 1)
    for plane in range(depth):
        put_plane(
            whole.at[plane],
            own[plane],
            band[plane, :ROWS],
            side[plane, :width],
            corner[plane, :ROWS],
        )
        put_plane(
            later.at[plane],
            noise_scale * inc[0, plane],
            noise_scale * band[plane, ROWS:],
            noise_scale * side[plane, width:],
            noise_scale * corner[plane, ROWS:],
        )
    at = jnp.where(upward(), depth - SWEEPS, 0)
    half = quarter.shape[0] - SWEEPS
    at_half = jnp.where(upward(), half, 0)
    for target, start, begin in (
        (first, at, at_half),
        (second, depth - SWEEPS - at, half - at_half),
    ):
        for index in range(SWEEPS):
            plane = start + index
            target[index * ROWS : (index + 1) * ROWS] = band[plane, :ROWS]
            packed = jnp.zeros((ROWS, LANES), jnp.float32)
            for tile in range(width // ROWS + 1):
                rows = side[plane, tile * ROWS : (tile + 1) * ROWS]
                if tile == width // ROWS:
                    rows = corner[plane, :ROWS]
                moved = pltpu.roll(rows, ROWS // 2 + tile * ROWS, 1)
                packed = jnp.where(lane // ROWS == tile, moved, packed)
            target[
                SWEEPS * ROWS : (SWEEPS + 1) * ROWS, index * LANES : (index + 1) * LANES
            ] = packed
        pack_rows(quarter[pl.ds(begin, SWEEPS)], target, (SWEEPS + 1) * ROWS)


def beside(center, before, after, rows):
    middle = center[:, rows]
    lane = lax.broadcasted_iota(jnp.int32, middle.shape, 2)
    back = pltpu.roll(middle, 1, 2)
    ahead = pltpu.roll(middle, LANES - 1, 2)
    back = jnp.where(lane == 0, jnp.concatenate([back[-1:], back[:-1]], axis=0), back)
    ahead = jnp.where(lane == LANES - 1, jnp.concatenate([ahead[1:], ahead[:1]], axis=0), ahead)
    total = center[:, rows.start - 1 : rows.stop - 1] + center[:, rows.start + 1 : rows.stop + 1]
    total = total + back + ahead
    if before is not None:
        total = total + before[:, rows]
    if after is not None:
        total = total + after[:, rows]
    return total


def chunks(width):
    for start in range(TOP, CELLS + width + ROWS, CHUNK):
        yield slice(start, start + CHUNK)


INVERSE = 1.0 / (1.0 + 6.0 * fine_coupling)


def sweep(target, right, center, before, after, width, finish=None):
    for rows in chunks(width):
        total = beside(center, before, after, rows)
        value = (right[:, rows] + fine_coupling * total) * INVERSE
        target[:, rows] = value if finish is None else finish(value, rows)


def forced(later):
    def finish(value, rows):
        return value + fine_step * (value - value * value * value) + later[:, rows]

    return finish


def inner_kernel(whole, later, mid, state):
    depth = whole.shape[0]
    width = whole.shape[2] - 2 * CELLS
    for plane in range(1, depth - 1):
        sweep(
            mid.at[plane - 1],
            whole.at[plane],
            whole.at[plane],
            whole.at[plane - 1],
            whole.at[plane + 1],
            width,
        )
    for plane in range(2, depth - 2):
        sweep(
            state.at[plane - 2],
            whole.at[plane],
            mid.at[plane - 1],
            mid.at[plane - 2],
            mid.at[plane],
            width,
            forced(later.at[plane]),
        )


def outer_kernel(
    whole, later, mid, planes_one, planes_two, strip_one, strip_two, edge, send_one, send_two, halo, part
):
    depth = whole.shape[0]
    width = planes_one.shape[1]
    up = upward()
    for planes, strip, send, top in (
        (planes_one, strip_one, send_one, up),
        (planes_two, strip_two, send_two, jnp.logical_not(up)),
    ):
        for index in range(SWEEPS):
            slot = jnp.where(top, index, SWEEPS - 1 - index)
            packed = strip[
                SWEEPS * ROWS : (SWEEPS + 1) * ROWS, index * LANES : (index + 1) * LANES
            ]
            tiles = [
                pltpu.roll(packed, LANES - ROWS // 2 - tile * ROWS, 1)
                for tile in range(width // ROWS + 1)
            ]
            put_plane(
                halo.at[slot],
                planes[index],
                strip[index * ROWS : (index + 1) * ROWS],
                jnp.concatenate(tiles[:-1], axis=0),
                tiles[-1],
            )
        zero = jnp.where(top, depth - 1, 0)
        one = jnp.where(top, depth - 2, 1)
        mid_one = jnp.where(top, depth - 3, 0)
        mid_two = jnp.where(top, depth - 4, 1)
        out = jnp.where(top, SWEEPS, 0)
        sweep(part.at[1], halo.at[0], halo.at[0], halo.at[1], whole.at[zero], width)
        sweep(part.at[0], whole.at[zero], whole.at[zero], halo.at[0], whole.at[one], width)
        sweep(
            edge.at[out],
            whole.at[zero],
            part.at[0],
            part.at[1],
            mid.at[mid_one],
            width,
            forced(later.at[zero]),
        )
        sweep(
            edge.at[out + 1],
            whole.at[one],
            mid.at[mid_one],
            part.at[0],
            mid.at[mid_two],
            width,
            forced(later.at[one]),
        )
        near = fine_coupling * INVERSE * INVERSE
        far = fine_coupling * near
        for rows in chunks(width):
            low, high = max(rows.start, CELLS), min(rows.stop, CELLS + width)
            if low >= high:
                continue
            rows = slice(low, high)
            to = slice(low - CELLS, high - CELLS)
            here = edge[out, :, rows]
            value = near * here + far * (
                2.0 * beside(edge.at[out], None, None, rows) + edge[out + 1, :, rows]
            )
            for tile in range(2):
                part_lanes = slice(tile * LANES, (tile + 1) * LANES)
                send[0, to, part_lanes] = value[tile]
                send[1, to, part_lanes] = far * here[tile]


def close_kernel(state, edge, out, mid):
    depth, width, _ = out.shape

    def at(plane):
        if plane < SWEEPS:
            return edge.at[plane]
        if plane < depth - SWEEPS:
            return state.at[plane - SWEEPS]
        return edge.at[SWEEPS + depth - 1 - plane]

    for plane in range(depth):
        sweep(
            mid.at[plane],
            at(plane),
            at(plane),
            at(plane - 1) if plane else None,
            at(plane + 1) if plane + 1 < depth else None,
            width,
        )
    for plane in range(depth):
        for start in range(CELLS, CELLS + width, CHUNK):
            rows = slice(start, start + CHUNK)
            total = beside(
                mid.at[plane],
                mid.at[plane - 1] if plane else None,
                mid.at[plane + 1] if plane + 1 < depth else None,
                rows,
            )
            here = at(plane)[:, rows]
            if plane in (0, depth - 1):
                total = total + (fine_coupling * INVERSE) * here
            value = (here + fine_coupling * total) * INVERSE
            to = slice(start - CELLS, start - CELLS + CHUNK)
            out[plane, to, :LANES] = value[0]
            out[plane, to, LANES:] = value[1]


def add_kernel(partial, one, two, out):
    depth = out.shape[0]
    up = upward()
    out[...] = partial[...]
    for add, top in ((one, up), (two, jnp.logical_not(up))):
        zero = jnp.where(top, depth - 1, 0)
        first = jnp.where(top, depth - 2, 1)
        out[zero] = out[zero] + add[0]
        out[first] = out[first] + add[1]


def column_kernel(quarter, one, two, column):
    planes, height = quarter.shape[0], quarter.shape[1]
    column[SWEEPS : SWEEPS + planes] = quarter[...]
    up = upward()
    for source, top in ((one, up), (two, jnp.logical_not(up))):
        at = jnp.where(top, SWEEPS + planes, 0)
        column[pl.ds(at, SWEEPS)] = unpack_rows(source, (SWEEPS + 1) * ROWS, SWEEPS, height)


def around(value, axes):
    total = None
    for axis in axes:
        count = value.shape[axis]
        both = pltpu.roll(value, 1, axis) + pltpu.roll(value, count - 1, axis)
        total = both if total is None else total + both
    return total


def coarse_kernel(mine, along, across, diagonal, out, src, mid):
    half_y, half_z = mine.shape[1], mine.shape[2]
    at_y, at_z = lax.axis_index("gy"), lax.axis_index("gz")
    for source, y, z in (
        (mine, at_y, at_z),
        (along, 1 - at_y, at_z),
        (across, at_y, 1 - at_z),
        (diagonal, 1 - at_y, 1 - at_z),
    ):
        rows = pl.ds(pl.multiple_of(y * half_y, half_y), half_y)
        lanes = pl.ds(pl.multiple_of(z * half_z, half_z), half_z)
        src[:, rows, lanes] = source[...]
    inverse = 1.0 / (1.0 + 6.0 * coarse_coupling)
    total = src.shape[0]

    def relax(fields, plane):
        sides = fields[plane + 1] + fields[plane - 1] + around(fields[plane], (0, 1))
        return (src[plane] + coarse_coupling * sides) * inverse

    for plane in range(1, total - 1):
        mid[plane] = relax(src, plane)
    for plane in range(SWEEPS, total - SWEEPS):
        out[plane - SWEEPS] = relax(mid, plane)


def swap_x(first, second):
    count = lax.axis_size("gx")
    even = [(i, i + 1 if i % 2 == 0 else i - 1) for i in range(count)]
    odd = [(i, (i + 1) % count if i % 2 else (i - 1) % count) for i in range(count)]
    second = lax.ppermute(second, "gx", odd)
    first = lax.ppermute(first, "gx", even)
    return first, second


def swap(value, axis):
    return lax.ppermute(value, axis, [(0, 1), (1, 0)])


def fused(fine_start, increments, coarse_start):
    depth, width, length = fine_start.shape
    half = (depth // 2, width // 2, length // 2)
    planes = (SWEEPS, width, length)
    padded = (3, width + 2 * CELLS, LANES)
    strips = ((SWEEPS + 1) * ROWS + SWEEPS * half[1] // 2, length)
    up = upward()
    own = reaction(fine_start, increments[0], fine_step)
    top, bottom = own[depth - SWEEPS :], own[:SWEEPS]
    first, second = jnp.where(up, top, bottom), jnp.where(up, bottom, top)
    planes_one, planes_two = swap_x(first, second)
    band, side, corner, quarter = call(
        open_kernel,
        [
            (depth, 2 * ROWS, length),
            (depth, 2 * width, LANES),
            (depth, 2 * ROWS, LANES),
            half,
        ],
        (own, increments, coarse_start),
        scratch=[pltpu.VMEM((length // LANES, depth // 2, width, LANES), jnp.float32)],
    )
    band_in = swap(band, "gy")
    corner_in = lax.ppermute(corner, ("gy", "gz"), [(0, 3), (3, 0), (1, 2), (2, 1)])
    side_in = swap(side, "gz")
    whole, later, first, second = call(
        spread_kernel,
        [(depth,) + padded, (depth,) + padded, strips, strips],
        (own, increments[STEPS - 1 :], quarter, band_in, side_in, corner_in),
    )
    strip_one, strip_two = swap_x(first, second)
    mid, state = call(inner_kernel, [(depth - 2,) + padded, (depth - 4,) + padded], (whole, later))
    edge, first, second = call(
        outer_kernel,
        [(2 * SWEEPS,) + padded, planes, planes],
        (whole, later, mid, planes_one, planes_two, strip_one, strip_two),
        scratch=[pltpu.VMEM((2,) + padded, jnp.float32)] * 2,
    )
    add_one, add_two = swap_x(first, second)
    (column,) = call(
        column_kernel, [(half[0] + 2 * SWEEPS,) + half[1:]], (quarter, strip_one, strip_two)
    )
    along = swap(column, "gy")
    across = swap(column, "gz")
    diagonal = swap(along, "gz")
    (partial,) = call(
        close_kernel,
        [fine_start.shape],
        (state, edge),
        scratch=[pltpu.VMEM((depth,) + padded, jnp.float32)],
    )
    slab = pltpu.VMEM((half[0] + 2 * SWEEPS,) + coarse_start.shape[1:], jnp.float32)
    (coarse_final,) = call(
        coarse_kernel,
        [coarse_start.shape],
        (column, along, across, diagonal),
        scratch=[slab, slab],
    )
    (fine_final,) = call(add_kernel, [fine_start.shape], (partial, add_one, add_two))
    return (fine_final, coarse_final)


def body(fine_start, increments, coarse_start):
    depth, width, length = fine_start.shape
    fits = (
        lax.axis_size("gy") == 2
        and lax.axis_size("gz") == 2
        and lax.axis_size("gx") % 2 == 0
        and (STEPS, SWEEPS) == (2, 2)
        and depth >= 2 * REACH
        and width % (4 * ROWS) == 0
        and width // ROWS + 1 <= LANES // ROWS
        and length == 2 * LANES
    )
    if not fits:
        return staged(fine_start, increments, coarse_start)
    return fused(fine_start, increments, coarse_start)


def solution(mesh):
    return jax.shard_map(
        body,
        mesh=mesh,
        in_specs=(
            P(("pairs", "gx"), "gy", "gz"),
            P(None, ("pairs", "gx"), "gy", "gz"),
            P(("pairs", "gx"), None, None),
        ),
        out_specs=(P(("pairs", "gx"), "gy", "gz"), P(("pairs", "gx"), None, None)),
        check_vma=False,
    )
```

```python
import jax
import jax.numpy as jnp
from jax import lax
from jax.experimental import pallas as pl
from jax.experimental.pallas import tpu as pltpu
from jax.sharding import PartitionSpec as P


STEPS = 2
SWEEPS = 2


noise_scale = 0.3
fine_step = 0.2
coarse_step = 0.4
fine_coupling = 1.0
coarse_coupling = 0.5


def with_halo(value, sides, width):
    for axis, dim in sides:
        count, length = (lax.axis_size(axis), value.shape[dim])
        up = [(i, (i + 1) % count) for i in range(count)]
        down = [(j, i) for i, j in up]
        last = lax.slice_in_dim(value, length - width, length, axis=dim)
        first = lax.slice_in_dim(value, 0, width, axis=dim)
        before = lax.ppermute(last, axis, up)
        after = lax.ppermute(first, axis, down)
        value = jnp.concatenate([before, value, after], axis=dim)
    return value


def neighbours(padded):
    beside = padded[2:, 1:-1, 1:-1] + padded[:-2, 1:-1, 1:-1]
    beside = beside + padded[1:-1, 2:, 1:-1] + padded[1:-1, :-2, 1:-1]
    beside = beside + padded[1:-1, 1:-1, 2:] + padded[1:-1, 1:-1, :-2]
    return beside


def trimmed_box(source, margin):
    return source[
        margin : source.shape[0] - margin,
        margin : source.shape[1] - margin,
        margin : source.shape[2] - margin,
    ]


def reaction(state, forcing, step_size):
    return state + step_size * (state - state * state * state) + noise_scale * forcing


def relaxed(source, coupling, extend):
    padded = extend(source, SWEEPS)
    fields = padded
    for sweep_index in range(SWEEPS):
        fields = (trimmed_box(padded, sweep_index + 1) + coupling * neighbours(fields)) / (
            1.0 + 6.0 * coupling
        )
    return fields


def fine_halo(source, width):
    return with_halo(source, (("gx", 0), ("gy", 1), ("gz", 2)), width)


def slab_halo(source, width):
    extended = with_halo(source, (("gx", 0),), width)
    return jnp.pad(extended, ((0, 0), (width, width), (width, width)), mode="wrap")


def assemble(stacked):
    count_y = lax.axis_size("gy")
    count_z = lax.axis_size("gz")
    depth_x, width_y, width_z = (stacked.shape[1], stacked.shape[2], stacked.shape[3])
    blocks = stacked.reshape(count_y, count_z, depth_x, width_y, width_z)
    return blocks.transpose(2, 0, 3, 1, 4).reshape(depth_x, count_y * width_y, count_z * width_z)


def pair_sum(length):
    fine = lax.broadcasted_iota(jnp.int32, (length, length // 2), 0)
    coarse = lax.broadcasted_iota(jnp.int32, (length, length // 2), 1)
    return (fine // 2 == coarse).astype(jnp.float32)


def staged(fine_start, increments, coarse_start):
    state = fine_start
    for step_index in range(STEPS):
        state = relaxed(
            reaction(state, increments[step_index], fine_step), fine_coupling, fine_halo
        )
    depth_x, width_y, width_z = increments.shape[1:]
    layers = increments.reshape(STEPS, depth_x // 2, 2, width_y, width_z).sum(axis=(0, 2))
    rows = lax.dot_general(
        layers.reshape(-1, width_z), pair_sum(width_z), (((1,), (0,)), ((), ())), precision="highest"
    ).reshape(depth_x // 2, width_y, width_z // 2)
    partial_value = 0.125 * jnp.einsum("ab,xbz->xaz", pair_sum(width_y).T, rows, precision="highest")
    slab_noise = assemble(lax.all_gather(partial_value[None], ("gy", "gz"), axis=0, tiled=True))
    coarse_final = relaxed(
        reaction(coarse_start, slab_noise, coarse_step), coarse_coupling, slab_halo
    )
    return (state, coarse_final)


LANES = 128
ROWS = 8
REACH = STEPS * SWEEPS

TOP = ROWS
CELLS = 2 * ROWS
CHUNK = 2 * ROWS


def call(kernel, outs, args, scratch=(), inputs=None, places=None, alias=None, flops=2000000):
    return pl.pallas_call(
        kernel,
        out_shape=[jax.ShapeDtypeStruct(shape, jnp.float32) for shape in outs],
        in_specs=inputs or [pl.BlockSpec(memory_space=pltpu.VMEM)] * len(args),
        out_specs=places or [pl.BlockSpec(memory_space=pltpu.VMEM)] * len(outs),
        input_output_aliases=alias or {},
        scratch_shapes=list(scratch),
        compiler_params=pltpu.CompilerParams(vmem_limit_bytes=16 * 1024 * 1024),
        cost_estimate=pl.CostEstimate(flops=flops, bytes_accessed=1000000, transcendentals=0),
    )(*args)


def edge_rows(value):
    length = value.shape[1]
    row = lax.broadcasted_iota(jnp.int32, (value.shape[0], ROWS, value.shape[2]), 1)
    return jnp.where(row < ROWS // 2, value[:, :ROWS], value[:, length - ROWS :])


def edge_lanes(value):
    length = value.shape[2]
    lane = lax.broadcasted_iota(jnp.int32, value.shape[:2] + (LANES,), 2)
    return jnp.where(lane < LANES // 2, value[:, :, :LANES], value[:, :, length - LANES :])


def upward():
    return lax.axis_index("gx") % 2 == 0


def pack_rows(quarter, target, first):
    for tile in range(quarter.shape[0] * quarter.shape[1] // (2 * ROWS)):
        plane, at = divmod(tile * 2 * ROWS, quarter.shape[1])
        rows = slice(first + tile * ROWS, first + (tile + 1) * ROWS)
        target[rows, :LANES] = quarter[plane, at : at + ROWS]
        target[rows, LANES:] = quarter[plane, at + ROWS : at + 2 * ROWS]


def unpack_rows(source, first, planes, height):
    parts = []
    for tile in range(planes * height // (2 * ROWS)):
        rows = slice(first + tile * ROWS, first + (tile + 1) * ROWS)
        parts += [source[rows, :LANES], source[rows, LANES:]]
    return jnp.concatenate(parts, axis=0).reshape(planes, height, LANES)


def paired(value):
    row = lax.broadcasted_iota(jnp.int32, value.shape[1:], 0)
    outer = (row < SWEEPS) | (row >= ROWS - SWEEPS)
    for plane in range(0, value.shape[0], 2):
        yield jnp.where(outer, value[plane], pltpu.roll(value[plane + 1], ROWS // 2, 0))


def gathered(tiles):
    lane = lax.broadcasted_iota(jnp.int32, (ROWS, LANES), 1)
    packed = jnp.zeros((ROWS, LANES), jnp.float32)
    for index in range(tiles.shape[0]):
        moved = pltpu.roll(tiles[index], ROWS // 2 + index * ROWS, 1)
        packed = jnp.where(lane // ROWS == index, moved, packed)
    return packed


def spread_out(packed, index):
    return pltpu.roll(packed, LANES - ROWS // 2 - index * ROWS, 1)


def halo_kernel(own, inc, band, side, corner):
    depth = own.shape[0]
    band[:depth] = edge_rows(own[...])
    for index, tile in enumerate(paired(edge_rows(inc[1]))):
        band[depth + index] = tile
    side[:depth] = edge_lanes(own[...])
    side[depth:] = edge_lanes(inc[1])
    corner[...] = gathered(edge_lanes(band[...]))


def restrict_kernel(inc, coarse, quarter, pairs):
    _, depth, width, length = inc.shape
    half_y, half_z = width // 2, length // 2
    layers = (inc[0] + inc[1]).reshape(depth // 2, 2, width, length)
    layers = layers[:, 0] + layers[:, 1]
    parts = []
    for tile in range(length // LANES):
        pairs[tile] = layers[:, :, tile * LANES : (tile + 1) * LANES]
        parts.append(
            pairs[tile, :, pl.ds(0, half_y, 2), :] + pairs[tile, :, pl.ds(1, half_y, 2), :]
        )
    rows = jnp.concatenate(parts, axis=2)
    summed = jnp.dot(
        rows.reshape(-1, length),
        pair_sum(length),
        precision=lax.Precision.HIGHEST,
        preferred_element_type=jnp.float32,
    ).reshape(depth // 2, half_y, half_z)
    at_y = pl.multiple_of(lax.axis_index("gy") * half_y, half_y)
    at_z = pl.multiple_of(lax.axis_index("gz") * half_z, half_z)
    start = coarse[:, pl.ds(at_y, half_y), pl.ds(at_z, half_z)]
    quarter[...] = reaction(start, 0.125 * summed, coarse_step)


def put_plane(target, cells, band, side, corner):
    width = cells.shape[0]
    for tile, part in enumerate((slice(0, LANES), slice(LANES, 2 * LANES))):
        target[tile, TOP:CELLS] = band[:, part]
        target[tile, CELLS : CELLS + width] = cells[:, part]
        target[tile, CELLS + width : CELLS + width + ROWS] = band[:, part]
    target[2, TOP:CELLS] = corner
    target[2, CELLS : CELLS + width] = side
    target[2, CELLS + width : CELLS + width + ROWS] = corner


def scale_kernel(inc, forcing):
    forcing[...] = noise_scale * inc[1]


def strip_kernel(quarter, band, side, corner, first, second):
    depth, width = side.shape[0] // 2, side.shape[1]
    at = jnp.where(upward(), depth - SWEEPS, 0)
    half = quarter.shape[0] - SWEEPS
    at_half = jnp.where(upward(), half, 0)
    ends = corner[...]
    for target, start, begin in (
        (first, at, at_half),
        (second, depth - SWEEPS - at, half - at_half),
    ):
        for index in range(SWEEPS):
            plane = start + index
            target[index * ROWS : (index + 1) * ROWS] = band[plane]
            tiles = side[plane].reshape(width // ROWS, ROWS, LANES)
            tiles = jnp.concatenate([tiles, spread_out(ends, plane)[None]], axis=0)
            target[
                SWEEPS * ROWS : (SWEEPS + 1) * ROWS, index * LANES : (index + 1) * LANES
            ] = gathered(tiles)
        pack_rows(quarter[pl.ds(begin, SWEEPS)], target, (SWEEPS + 1) * ROWS)


def spread_kernel(own, forcing, band, side, corner, whole, later):
    depth = own.shape[0]
    packed = corner[...]
    for plane in range(depth):
        put_plane(
            whole.at[plane], own[plane], band[plane], side[plane], spread_out(packed, plane)
        )
        tile = depth + plane // 2
        rows, ends = band[tile], spread_out(packed, tile)
        if plane % 2:
            rows, ends = pltpu.roll(rows, ROWS // 2, 0), pltpu.roll(ends, ROWS // 2, 0)
        put_plane(
            later.at[plane],
            forcing[plane],
            noise_scale * rows,
            noise_scale * side[depth + plane],
            noise_scale * ends,
        )


def beside(center, before, after, rows):
    middle = center[:, rows]
    lane = lax.broadcasted_iota(jnp.int32, middle.shape, 2)
    back = pltpu.roll(middle, 1, 2)
    ahead = pltpu.roll(middle, LANES - 1, 2)
    back = jnp.where(lane == 0, jnp.concatenate([back[-1:], back[:-1]], axis=0), back)
    ahead = jnp.where(lane == LANES - 1, jnp.concatenate([ahead[1:], ahead[:1]], axis=0), ahead)
    total = center[:, rows.start - 1 : rows.stop - 1] + center[:, rows.start + 1 : rows.stop + 1]
    total = total + back + ahead
    if before is not None:
        total = total + before[:, rows]
    if after is not None:
        total = total + after[:, rows]
    return total


def chunks(width):
    for start in range(TOP, CELLS + width + ROWS, CHUNK):
        yield slice(start, start + CHUNK)


INVERSE = 1.0 / (1.0 + 6.0 * fine_coupling)


def sweep(target, right, center, before, after, width, finish=None):
    for rows in chunks(width):
        total = beside(center, before, after, rows)
        value = (right[:, rows] + fine_coupling * total) * INVERSE
        target[:, rows] = value if finish is None else finish(value, rows)


def forced(later):
    def finish(value, rows):
        return value + fine_step * (value - value * value * value) + later[:, rows]

    return finish


def inner_kernel(whole, later, mid, state):
    depth = whole.shape[0]
    width = whole.shape[2] - 2 * CELLS
    for plane in range(1, depth - 1):
        sweep(
            mid.at[plane - 1],
            whole.at[plane],
            whole.at[plane],
            whole.at[plane - 1],
            whole.at[plane + 1],
            width,
        )
    for plane in range(2, depth - 2):
        sweep(
            state.at[plane - 2],
            whole.at[plane],
            mid.at[plane - 1],
            mid.at[plane - 2],
            mid.at[plane],
            width,
            forced(later.at[plane]),
        )


def outer_kernel(whole, later, mid, low, high, strip, edge, send, halo, part, top):
    depth = whole.shape[0]
    width = low.shape[1]
    for index in range(SWEEPS):
        slot = jnp.where(top, index, SWEEPS - 1 - index)
        packed = strip[SWEEPS * ROWS : (SWEEPS + 1) * ROWS, index * LANES : (index + 1) * LANES]
        tiles = [spread_out(packed, tile) for tile in range(width // ROWS + 1)]
        put_plane(
            halo.at[slot],
            jnp.where(top, high[index], low[index]),
            strip[index * ROWS : (index + 1) * ROWS],
            jnp.concatenate(tiles[:-1], axis=0),
            tiles[-1],
        )
    zero = jnp.where(top, depth - 1, 0)
    one = jnp.where(top, depth - 2, 1)
    mid_one = jnp.where(top, depth - 3, 0)
    mid_two = jnp.where(top, depth - 4, 1)
    sweep(part.at[1], halo.at[0], halo.at[0], halo.at[1], whole.at[zero], width)
    sweep(part.at[0], whole.at[zero], whole.at[zero], halo.at[0], whole.at[one], width)
    sweep(
        edge.at[0],
        whole.at[zero],
        part.at[0],
        part.at[1],
        mid.at[mid_one],
        width,
        forced(later.at[zero]),
    )
    sweep(
        edge.at[1],
        whole.at[one],
        mid.at[mid_one],
        part.at[0],
        mid.at[mid_two],
        width,
        forced(later.at[one]),
    )
    near = fine_coupling * INVERSE * INVERSE
    far = fine_coupling * near
    for rows in chunks(width):
        low, high = max(rows.start, CELLS), min(rows.stop, CELLS + width)
        if low >= high:
            continue
        rows = slice(low, high)
        to = slice(low - CELLS, high - CELLS)
        here = edge[0, :, rows]
        value = near * here + far * (
            2.0 * beside(edge.at[0], None, None, rows) + edge[1, :, rows]
        )
        for tile in range(2):
            lanes = slice(tile * LANES, (tile + 1) * LANES)
            send[0, to, lanes] = value[tile]
            send[1, to, lanes] = far * here[tile]


def first_outer(whole, later, mid, low, high, strip, edge, send, halo, part):
    outer_kernel(
        whole, later, mid, low, high, strip, edge, send, halo, part, jnp.logical_not(upward())
    )


def second_outer(whole, later, mid, low, high, strip, edge, send, halo, part):
    outer_kernel(whole, later, mid, low, high, strip, edge, send, halo, part, upward())


def close_kernel(state, edge_one, edge_two, out, rim, mid, rows_low, rows_high, inner, sems):
    depth, width, _ = out.shape
    up = upward()

    @pl.when(up)
    def _():
        rows_high[...] = edge_one[...]
        rows_low[...] = edge_two[...]

    @pl.when(jnp.logical_not(up))
    def _():
        rows_low[...] = edge_one[...]
        rows_high[...] = edge_two[...]

    def at(plane):
        if plane < SWEEPS:
            return rows_low.at[plane]
        if plane < depth - SWEEPS:
            return state.at[plane - SWEEPS]
        return rows_high.at[depth - 1 - plane]

    for plane in range(depth):
        sweep(
            mid.at[plane],
            at(plane),
            at(plane),
            at(plane - 1) if plane else None,
            at(plane + 1) if plane + 1 < depth else None,
            width,
        )
    for plane in [*range(SWEEPS, depth - SWEEPS), 0, 1, depth - 2, depth - 1]:
        for start in range(CELLS, CELLS + width, CHUNK):
            rows = slice(start, start + CHUNK)
            total = beside(
                mid.at[plane],
                mid.at[plane - 1] if plane else None,
                mid.at[plane + 1] if plane + 1 < depth else None,
                rows,
            )
            here = at(plane)[:, rows]
            if plane in (0, depth - 1):
                total = total + (fine_coupling * INVERSE) * here
            value = (here + fine_coupling * total) * INVERSE
            to = slice(start - CELLS, start - CELLS + CHUNK)
            target = inner.at[plane - SWEEPS]
            if plane < SWEEPS:
                target = rim.at[plane]
            if plane >= depth - SWEEPS:
                target = rim.at[plane - depth + 2 * SWEEPS]
            target[to, :LANES] = value[0]
            target[to, LANES:] = value[1]
        if plane == depth - SWEEPS - 1:
            copy = pltpu.make_async_copy(
                inner, out.at[pl.ds(SWEEPS, depth - 2 * SWEEPS)], sems.at[0]
            )
            copy.start()
    copy.wait()


def add_kernel(partial, rim, one, two, out, low, high, sems):
    depth = out.shape[0]
    up = upward()

    def place(add_low, add_high):
        low[0] = rim[0] + add_low[0]
        low[1] = rim[1] + add_low[1]
        high[0] = rim[2] + add_high[1]
        high[1] = rim[3] + add_high[0]

    @pl.when(up)
    def _():
        place(two, one)

    @pl.when(jnp.logical_not(up))
    def _():
        place(one, two)

    copies = (
        pltpu.make_async_copy(low, out.at[pl.ds(0, SWEEPS)], sems.at[0]),
        pltpu.make_async_copy(high, out.at[pl.ds(depth - SWEEPS, SWEEPS)], sems.at[1]),
    )
    for copy in copies:
        copy.start()
    for copy in copies:
        copy.wait()


def column_kernel(one, two, column):
    height = column.shape[1]
    up = upward()
    for source, top in ((one, up), (two, jnp.logical_not(up))):
        at = jnp.where(top, SWEEPS, 0)
        column[pl.ds(at, SWEEPS)] = unpack_rows(source, (SWEEPS + 1) * ROWS, SWEEPS, height)


def around(value, axes):
    total = None
    for axis in axes:
        count = value.shape[axis]
        both = pltpu.roll(value, 1, axis) + pltpu.roll(value, count - 1, axis)
        total = both if total is None else total + both
    return total


def coarse_kernel(*refs):
    blocks, (out, src, mid) = refs[:8], refs[8:]
    planes, half_y, half_z = blocks[0].shape
    at_y, at_z = lax.axis_index("gy"), lax.axis_index("gz")
    places = ((at_y, at_z), (1 - at_y, at_z), (at_y, 1 - at_z), (1 - at_y, 1 - at_z))
    for source, rim, (y, z) in zip(blocks[:4], blocks[4:], places):
        rows = pl.ds(pl.multiple_of(y * half_y, half_y), half_y)
        lanes = pl.ds(pl.multiple_of(z * half_z, half_z), half_z)
        src[:SWEEPS, rows, lanes] = rim[:SWEEPS]
        src[SWEEPS : SWEEPS + planes, rows, lanes] = source[...]
        src[SWEEPS + planes :, rows, lanes] = rim[SWEEPS:]
    inverse = 1.0 / (1.0 + 6.0 * coarse_coupling)
    total = src.shape[0]

    def relax(fields, plane):
        sides = fields[plane + 1] + fields[plane - 1] + around(fields[plane], (0, 1))
        return (src[plane] + coarse_coupling * sides) * inverse

    for plane in range(1, total - 1):
        mid[plane] = relax(src, plane)
    for plane in range(SWEEPS, total - SWEEPS):
        out[plane - SWEEPS] = relax(mid, plane)


def pairs_x():
    count = lax.axis_size("gx")
    even = [(i, i + 1 if i % 2 == 0 else i - 1) for i in range(count)]
    odd = [(i, (i + 1) % count if i % 2 else (i - 1) % count) for i in range(count)]
    return even, odd


def swap_x(first, second):
    even, odd = pairs_x()
    second = lax.ppermute(second, "gx", odd)
    first = lax.ppermute(first, "gx", even)
    return first, second


def swap(value, axis):
    return lax.ppermute(value, axis, [(0, 1), (1, 0)])


def swap_yz(band, side, corner):
    band = swap(band, "gy")
    corner = lax.ppermute(corner, ("gy", "gz"), [(0, 3), (3, 0), (1, 2), (2, 1)])
    side = swap(side, "gz")
    return band, side, corner


def gather_yz(value):
    along = swap(value, "gy")
    across = swap(value, "gz")
    diagonal = swap(along, "gz")
    return value, along, across, diagonal


def fused(fine_start, increments, coarse_start):
    depth, width, length = fine_start.shape
    half = (depth // 2, width // 2, length // 2)
    planes = (SWEEPS, width, length)
    padded = (3, width + 2 * CELLS, LANES)
    strips = ((SWEEPS + 1) * ROWS + SWEEPS * half[1] // 2, length)
    own = reaction(fine_start, increments[0], fine_step)
    even, odd = pairs_x()
    count = lax.axis_size("gx")
    rise = [(i, (i + 1) % count) for i in range(count)]
    fall = [(j, i) for i, j in rise]
    low = lax.ppermute(own[depth - SWEEPS :], "gx", rise)
    tiles = depth + depth // 2
    band, side, corner = call(
        halo_kernel,
        [(tiles, ROWS, length), (2 * depth, width, LANES), (ROWS, LANES)],
        (own, increments),
    )
    halo_in = swap_yz(band, side, corner)
    high = lax.ppermute(own[:SWEEPS], "gx", fall)
    (quarter,) = call(
        restrict_kernel,
        [half],
        (increments, coarse_start),
        scratch=[pltpu.VMEM((length // LANES, depth // 2, width, LANES), jnp.float32)],
    )
    first, second = call(strip_kernel, [strips, strips], (quarter,) + halo_in)
    strip_one, strip_two = swap_x(first, second)
    (forcing,) = call(scale_kernel, [fine_start.shape], (increments,))
    whole, later = call(
        spread_kernel,
        [(depth,) + padded, (depth,) + padded],
        (own, forcing) + halo_in,
    )
    quarters = gather_yz(quarter)
    mid, state = call(inner_kernel, [(depth - 2,) + padded, (depth - 4,) + padded], (whole, later))

    def outer(kernel, *halo):
        return call(
            kernel,
            [(SWEEPS,) + padded, planes],
            (whole, later, mid) + halo,
            scratch=[pltpu.VMEM((SWEEPS,) + padded, jnp.float32)] * 2,
        )

    edge_two, second = outer(first_outer, low, high, strip_two)
    add_two = lax.ppermute(second, "gx", odd)
    edge_one, first = outer(second_outer, low, high, strip_one)
    add_one = lax.ppermute(first, "gx", even)
    (column,) = call(column_kernel, [(2 * SWEEPS,) + half[1:]], (strip_one, strip_two))
    columns = gather_yz(column)
    hbm = pl.BlockSpec(memory_space=pltpu.HBM)
    vmem = pl.BlockSpec(memory_space=pltpu.VMEM)
    partial, rim = call(
        close_kernel,
        [fine_start.shape, (2 * SWEEPS, width, length)],
        (state, edge_one, edge_two),
        scratch=[
            pltpu.VMEM((depth,) + padded, jnp.float32),
            pltpu.VMEM((SWEEPS,) + padded, jnp.float32),
            pltpu.VMEM((SWEEPS,) + padded, jnp.float32),
            pltpu.VMEM((depth - 2 * SWEEPS, width, length), jnp.float32),
            pltpu.SemaphoreType.DMA((1,)),
        ],
        places=[hbm, vmem],
    )
    slab = pltpu.VMEM((half[0] + 2 * SWEEPS,) + coarse_start.shape[1:], jnp.float32)
    (coarse_final,) = call(
        coarse_kernel, [coarse_start.shape], quarters + columns, scratch=[slab, slab]
    )
    (fine_final,) = call(
        add_kernel,
        [fine_start.shape],
        (partial, rim, add_one, add_two),
        inputs=[hbm, vmem, vmem, vmem],
        places=[hbm],
        alias={0: 0},
        scratch=[pltpu.VMEM(planes, jnp.float32)] * 2 + [pltpu.SemaphoreType.DMA((2,))],
    )
    return (fine_final, coarse_final)


def body(fine_start, increments, coarse_start):
    depth, width, length = fine_start.shape
    fits = (
        lax.axis_size("gy") == 2
        and lax.axis_size("gz") == 2
        and lax.axis_size("gx") % 2 == 0
        and (STEPS, SWEEPS) == (2, 2)
        and depth >= 2 * REACH
        and depth % 2 == 0
        and (depth + depth // 2) * ROWS <= LANES
        and width % (4 * ROWS) == 0
        and width // ROWS + 1 <= LANES // ROWS
        and length == 2 * LANES
    )
    if not fits:
        return staged(fine_start, increments, coarse_start)
    return fused(fine_start, increments, coarse_start)


def solution(mesh):
    return jax.shard_map(
        body,
        mesh=mesh,
        in_specs=(
            P(("pairs", "gx"), "gy", "gz"),
            P(None, ("pairs", "gx"), "gy", "gz"),
            P(("pairs", "gx"), None, None),
        ),
        out_specs=(P(("pairs", "gx"), "gy", "gz"), P(("pairs", "gx"), None, None)),
        check_vma=False,
    )
```

```python
import jax
import jax.numpy as jnp
from jax import lax
from jax.experimental import pallas as pl
from jax.experimental.pallas import tpu as pltpu
from jax.sharding import PartitionSpec as P


STEPS = 2
SWEEPS = 2


noise_scale = 0.3
fine_step = 0.2
coarse_step = 0.4
fine_coupling = 1.0
coarse_coupling = 0.5


def with_halo(value, sides, width):
    for axis, dim in sides:
        count, length = (lax.axis_size(axis), value.shape[dim])
        up = [(i, (i + 1) % count) for i in range(count)]
        down = [(j, i) for i, j in up]
        last = lax.slice_in_dim(value, length - width, length, axis=dim)
        first = lax.slice_in_dim(value, 0, width, axis=dim)
        before = lax.ppermute(last, axis, up)
        after = lax.ppermute(first, axis, down)
        value = jnp.concatenate([before, value, after], axis=dim)
    return value


def neighbours(padded):
    beside = padded[2:, 1:-1, 1:-1] + padded[:-2, 1:-1, 1:-1]
    beside = beside + padded[1:-1, 2:, 1:-1] + padded[1:-1, :-2, 1:-1]
    beside = beside + padded[1:-1, 1:-1, 2:] + padded[1:-1, 1:-1, :-2]
    return beside


def trimmed_box(source, margin):
    return source[
        margin : source.shape[0] - margin,
        margin : source.shape[1] - margin,
        margin : source.shape[2] - margin,
    ]


def reaction(state, forcing, step_size):
    return state + step_size * (state - state * state * state) + noise_scale * forcing


def relaxed(source, coupling, extend):
    padded = extend(source, SWEEPS)
    fields = padded
    for sweep_index in range(SWEEPS):
        fields = (trimmed_box(padded, sweep_index + 1) + coupling * neighbours(fields)) / (
            1.0 + 6.0 * coupling
        )
    return fields


def fine_halo(source, width):
    return with_halo(source, (("gx", 0), ("gy", 1), ("gz", 2)), width)


def slab_halo(source, width):
    extended = with_halo(source, (("gx", 0),), width)
    return jnp.pad(extended, ((0, 0), (width, width), (width, width)), mode="wrap")


def assemble(stacked):
    count_y = lax.axis_size("gy")
    count_z = lax.axis_size("gz")
    depth_x, width_y, width_z = (stacked.shape[1], stacked.shape[2], stacked.shape[3])
    blocks = stacked.reshape(count_y, count_z, depth_x, width_y, width_z)
    return blocks.transpose(2, 0, 3, 1, 4).reshape(depth_x, count_y * width_y, count_z * width_z)


def pair_sum(length):
    fine = lax.broadcasted_iota(jnp.int32, (length, length // 2), 0)
    coarse = lax.broadcasted_iota(jnp.int32, (length, length // 2), 1)
    return (fine // 2 == coarse).astype(jnp.float32)


def staged(fine_start, increments, coarse_start):
    state = fine_start
    for step_index in range(STEPS):
        state = relaxed(
            reaction(state, increments[step_index], fine_step), fine_coupling, fine_halo
        )
    depth_x, width_y, width_z = increments.shape[1:]
    layers = increments.reshape(STEPS, depth_x // 2, 2, width_y, width_z).sum(axis=(0, 2))
    rows = lax.dot_general(
        layers.reshape(-1, width_z), pair_sum(width_z), (((1,), (0,)), ((), ())), precision="highest"
    ).reshape(depth_x // 2, width_y, width_z // 2)
    partial_value = 0.125 * jnp.einsum("ab,xbz->xaz", pair_sum(width_y).T, rows, precision="highest")
    slab_noise = assemble(lax.all_gather(partial_value[None], ("gy", "gz"), axis=0, tiled=True))
    coarse_final = relaxed(
        reaction(coarse_start, slab_noise, coarse_step), coarse_coupling, slab_halo
    )
    return (state, coarse_final)


LANES = 128
ROWS = 8
REACH = STEPS * SWEEPS

TOP = ROWS
CELLS = 2 * ROWS
CHUNK = 2 * ROWS


def call(kernel, outs, args, scratch=(), inputs=None, places=None, alias=None, flops=2000000):
    return pl.pallas_call(
        kernel,
        out_shape=[jax.ShapeDtypeStruct(shape, jnp.float32) for shape in outs],
        in_specs=inputs or [pl.BlockSpec(memory_space=pltpu.VMEM)] * len(args),
        out_specs=places or [pl.BlockSpec(memory_space=pltpu.VMEM)] * len(outs),
        input_output_aliases=alias or {},
        scratch_shapes=list(scratch),
        compiler_params=pltpu.CompilerParams(vmem_limit_bytes=16 * 1024 * 1024),
        cost_estimate=pl.CostEstimate(flops=flops, bytes_accessed=1000000, transcendentals=0),
    )(*args)


def edge_rows(value):
    length = value.shape[1]
    row = lax.broadcasted_iota(jnp.int32, (value.shape[0], ROWS, value.shape[2]), 1)
    return jnp.where(row < ROWS // 2, value[:, :ROWS], value[:, length - ROWS :])


def edge_lanes(value):
    length = value.shape[2]
    lane = lax.broadcasted_iota(jnp.int32, value.shape[:2] + (LANES,), 2)
    return jnp.where(lane < LANES // 2, value[:, :, :LANES], value[:, :, length - LANES :])


def upward():
    return lax.axis_index("gx") % 2 == 0


def pack_rows(quarter, target, first):
    for tile in range(quarter.shape[0] * quarter.shape[1] // (2 * ROWS)):
        plane, at = divmod(tile * 2 * ROWS, quarter.shape[1])
        rows = slice(first + tile * ROWS, first + (tile + 1) * ROWS)
        target[rows, :LANES] = quarter[plane, at : at + ROWS]
        target[rows, LANES:] = quarter[plane, at + ROWS : at + 2 * ROWS]


def unpack_rows(source, first, planes, height):
    parts = []
    for tile in range(planes * height // (2 * ROWS)):
        rows = slice(first + tile * ROWS, first + (tile + 1) * ROWS)
        parts += [source[rows, :LANES], source[rows, LANES:]]
    return jnp.concatenate(parts, axis=0).reshape(planes, height, LANES)


def paired(value):
    row = lax.broadcasted_iota(jnp.int32, value.shape[1:], 0)
    outer = (row < SWEEPS) | (row >= ROWS - SWEEPS)
    for plane in range(0, value.shape[0], 2):
        yield jnp.where(outer, value[plane], pltpu.roll(value[plane + 1], ROWS // 2, 0))


def gathered(tiles):
    lane = lax.broadcasted_iota(jnp.int32, (ROWS, LANES), 1)
    packed = jnp.zeros((ROWS, LANES), jnp.float32)
    for index in range(tiles.shape[0]):
        moved = pltpu.roll(tiles[index], ROWS // 2 + index * ROWS, 1)
        packed = jnp.where(lane // ROWS == index, moved, packed)
    return packed


def spread_out(packed, index):
    return pltpu.roll(packed, LANES - ROWS // 2 - index * ROWS, 1)


def halo_kernel(own, inc, band, more, side, corner):
    depth = own.shape[0]
    band[...] = edge_rows(own[...])
    for index, tile in enumerate(paired(edge_rows(inc[1]))):
        more[index] = tile
    side[:depth] = edge_lanes(own[...])
    side[depth:] = edge_lanes(inc[1])
    corner[...] = gathered(jnp.concatenate([edge_lanes(band[...]), edge_lanes(more[...])], axis=0))


def restrict_kernel(inc, coarse, quarter, pairs):
    _, depth, width, length = inc.shape
    half_y, half_z = width // 2, length // 2
    layers = (inc[0] + inc[1]).reshape(depth // 2, 2, width, length)
    layers = layers[:, 0] + layers[:, 1]
    parts = []
    for tile in range(length // LANES):
        pairs[tile] = layers[:, :, tile * LANES : (tile + 1) * LANES]
        parts.append(
            pairs[tile, :, pl.ds(0, half_y, 2), :] + pairs[tile, :, pl.ds(1, half_y, 2), :]
        )
    rows = jnp.concatenate(parts, axis=2)
    summed = jnp.dot(
        rows.reshape(-1, length),
        pair_sum(length),
        precision=lax.Precision.HIGHEST,
        preferred_element_type=jnp.float32,
    ).reshape(depth // 2, half_y, half_z)
    at_y = pl.multiple_of(lax.axis_index("gy") * half_y, half_y)
    at_z = pl.multiple_of(lax.axis_index("gz") * half_z, half_z)
    start = coarse[:, pl.ds(at_y, half_y), pl.ds(at_z, half_z)]
    quarter[...] = reaction(start, 0.125 * summed, coarse_step)


def put_plane(target, cells, band, side, corner):
    width = cells.shape[0]
    for tile, part in enumerate((slice(0, LANES), slice(LANES, 2 * LANES))):
        target[tile, TOP:CELLS] = band[:, part]
        target[tile, CELLS : CELLS + width] = cells[:, part]
        target[tile, CELLS + width : CELLS + width + ROWS] = band[:, part]
    target[2, TOP:CELLS] = corner
    target[2, CELLS : CELLS + width] = side
    target[2, CELLS + width : CELLS + width + ROWS] = corner


def scale_kernel(inc, forcing):
    forcing[...] = noise_scale * inc[1]


def strip_kernel(quarter, band, side, corner, first, second):
    depth, width = side.shape[0] // 2, side.shape[1]
    at = jnp.where(upward(), depth - SWEEPS, 0)
    half = quarter.shape[0] - SWEEPS
    at_half = jnp.where(upward(), half, 0)
    ends = corner[...]
    for target, start, begin in (
        (first, at, at_half),
        (second, depth - SWEEPS - at, half - at_half),
    ):
        for index in range(SWEEPS):
            plane = start + index
            target[index * ROWS : (index + 1) * ROWS] = band[plane]
            tiles = side[plane].reshape(width // ROWS, ROWS, LANES)
            tiles = jnp.concatenate([tiles, spread_out(ends, plane)[None]], axis=0)
            target[
                SWEEPS * ROWS : (SWEEPS + 1) * ROWS, index * LANES : (index + 1) * LANES
            ] = gathered(tiles)
        pack_rows(quarter[pl.ds(begin, SWEEPS)], target, (SWEEPS + 1) * ROWS)


def spread_kernel(own, forcing, band, more, side, corner, whole, later):
    depth = own.shape[0]
    packed = corner[...]
    for plane in range(depth):
        put_plane(
            whole.at[plane], own[plane], band[plane], side[plane], spread_out(packed, plane)
        )
        tile = depth + plane // 2
        rows, ends = more[plane // 2], spread_out(packed, tile)
        if plane % 2:
            rows, ends = pltpu.roll(rows, ROWS // 2, 0), pltpu.roll(ends, ROWS // 2, 0)
        put_plane(
            later.at[plane],
            forcing[plane],
            noise_scale * rows,
            noise_scale * side[depth + plane],
            noise_scale * ends,
        )


def beside(center, before, after, rows):
    middle = center[:, rows]
    lane = lax.broadcasted_iota(jnp.int32, middle.shape, 2)
    back = pltpu.roll(middle, 1, 2)
    ahead = pltpu.roll(middle, LANES - 1, 2)
    back = jnp.where(lane == 0, jnp.concatenate([back[-1:], back[:-1]], axis=0), back)
    ahead = jnp.where(lane == LANES - 1, jnp.concatenate([ahead[1:], ahead[:1]], axis=0), ahead)
    total = center[:, rows.start - 1 : rows.stop - 1] + center[:, rows.start + 1 : rows.stop + 1]
    total = total + back + ahead
    if before is not None:
        total = total + before[:, rows]
    if after is not None:
        total = total + after[:, rows]
    return total


def chunks(width):
    for start in range(TOP, CELLS + width + ROWS, CHUNK):
        yield slice(start, start + CHUNK)


INVERSE = 1.0 / (1.0 + 6.0 * fine_coupling)


def sweep(target, right, center, before, after, width, finish=None):
    for rows in chunks(width):
        total = beside(center, before, after, rows)
        value = (right[:, rows] + fine_coupling * total) * INVERSE
        target[:, rows] = value if finish is None else finish(value, rows)


def forced(later):
    def finish(value, rows):
        return value + fine_step * (value - value * value * value) + later[:, rows]

    return finish


def inner_kernel(whole, later, mid, state):
    depth = whole.shape[0]
    width = whole.shape[2] - 2 * CELLS
    for plane in range(1, depth - 1):
        sweep(
            mid.at[plane - 1],
            whole.at[plane],
            whole.at[plane],
            whole.at[plane - 1],
            whole.at[plane + 1],
            width,
        )
    for plane in range(2, depth - 2):
        sweep(
            state.at[plane - 2],
            whole.at[plane],
            mid.at[plane - 1],
            mid.at[plane - 2],
            mid.at[plane],
            width,
            forced(later.at[plane]),
        )


def outer_kernel(whole, later, mid, low, high, strip, edge, send, halo, part, top):
    depth = whole.shape[0]
    width = low.shape[1]
    for index in range(SWEEPS):
        slot = jnp.where(top, index, SWEEPS - 1 - index)
        packed = strip[SWEEPS * ROWS : (SWEEPS + 1) * ROWS, index * LANES : (index + 1) * LANES]
        tiles = [spread_out(packed, tile) for tile in range(width // ROWS + 1)]
        put_plane(
            halo.at[slot],
            jnp.where(top, high[index], low[index]),
            strip[index * ROWS : (index + 1) * ROWS],
            jnp.concatenate(tiles[:-1], axis=0),
            tiles[-1],
        )
    zero = jnp.where(top, depth - 1, 0)
    one = jnp.where(top, depth - 2, 1)
    mid_one = jnp.where(top, depth - 3, 0)
    mid_two = jnp.where(top, depth - 4, 1)
    sweep(part.at[1], halo.at[0], halo.at[0], halo.at[1], whole.at[zero], width)
    sweep(part.at[0], whole.at[zero], whole.at[zero], halo.at[0], whole.at[one], width)
    sweep(
        edge.at[0],
        whole.at[zero],
        part.at[0],
        part.at[1],
        mid.at[mid_one],
        width,
        forced(later.at[zero]),
    )
    sweep(
        edge.at[1],
        whole.at[one],
        mid.at[mid_one],
        part.at[0],
        mid.at[mid_two],
        width,
        forced(later.at[one]),
    )
    near = fine_coupling * INVERSE * INVERSE
    far = fine_coupling * near
    for rows in chunks(width):
        low, high = max(rows.start, CELLS), min(rows.stop, CELLS + width)
        if low >= high:
            continue
        rows = slice(low, high)
        to = slice(low - CELLS, high - CELLS)
        here = edge[0, :, rows]
        value = near * here + far * (
            2.0 * beside(edge.at[0], None, None, rows) + edge[1, :, rows]
        )
        for tile in range(2):
            lanes = slice(tile * LANES, (tile + 1) * LANES)
            send[0, to, lanes] = value[tile]
            send[1, to, lanes] = far * here[tile]


def first_outer(whole, later, mid, low, high, strip, edge, send, halo, part):
    outer_kernel(
        whole, later, mid, low, high, strip, edge, send, halo, part, jnp.logical_not(upward())
    )


def second_outer(whole, later, mid, low, high, strip, edge, send, halo, part):
    outer_kernel(whole, later, mid, low, high, strip, edge, send, halo, part, upward())


def close_kernel(state, edge_one, edge_two, out, rim, mid, rows_low, rows_high, inner, sems):
    depth, width, _ = out.shape
    up = upward()

    @pl.when(up)
    def _():
        rows_high[...] = edge_one[...]
        rows_low[...] = edge_two[...]

    @pl.when(jnp.logical_not(up))
    def _():
        rows_low[...] = edge_one[...]
        rows_high[...] = edge_two[...]

    def at(plane):
        if plane < SWEEPS:
            return rows_low.at[plane]
        if plane < depth - SWEEPS:
            return state.at[plane - SWEEPS]
        return rows_high.at[depth - 1 - plane]

    for plane in range(depth):
        sweep(
            mid.at[plane],
            at(plane),
            at(plane),
            at(plane - 1) if plane else None,
            at(plane + 1) if plane + 1 < depth else None,
            width,
        )
    for plane in [*range(SWEEPS, depth - SWEEPS), 0, 1, depth - 2, depth - 1]:
        for start in range(CELLS, CELLS + width, CHUNK):
            rows = slice(start, start + CHUNK)
            total = beside(
                mid.at[plane],
                mid.at[plane - 1] if plane else None,
                mid.at[plane + 1] if plane + 1 < depth else None,
                rows,
            )
            here = at(plane)[:, rows]
            if plane in (0, depth - 1):
                total = total + (fine_coupling * INVERSE) * here
            value = (here + fine_coupling * total) * INVERSE
            to = slice(start - CELLS, start - CELLS + CHUNK)
            target = inner.at[plane - SWEEPS]
            if plane < SWEEPS:
                target = rim.at[plane]
            if plane >= depth - SWEEPS:
                target = rim.at[plane - depth + 2 * SWEEPS]
            target[to, :LANES] = value[0]
            target[to, LANES:] = value[1]
        if plane == depth - SWEEPS - 1:
            copy = pltpu.make_async_copy(
                inner, out.at[pl.ds(SWEEPS, depth - 2 * SWEEPS)], sems.at[0]
            )
            copy.start()
    copy.wait()


def add_kernel(partial, rim, one, two, out, low, high, sems):
    depth = out.shape[0]
    up = upward()

    def place(add_low, add_high):
        low[0] = rim[0] + add_low[0]
        low[1] = rim[1] + add_low[1]
        high[0] = rim[2] + add_high[1]
        high[1] = rim[3] + add_high[0]

    @pl.when(up)
    def _():
        place(two, one)

    @pl.when(jnp.logical_not(up))
    def _():
        place(one, two)

    copies = (
        pltpu.make_async_copy(low, out.at[pl.ds(0, SWEEPS)], sems.at[0]),
        pltpu.make_async_copy(high, out.at[pl.ds(depth - SWEEPS, SWEEPS)], sems.at[1]),
    )
    for copy in copies:
        copy.start()
    for copy in copies:
        copy.wait()


def column_kernel(one, two, column):
    height = column.shape[1]
    up = upward()
    for source, top in ((one, up), (two, jnp.logical_not(up))):
        at = jnp.where(top, SWEEPS, 0)
        column[pl.ds(at, SWEEPS)] = unpack_rows(source, (SWEEPS + 1) * ROWS, SWEEPS, height)


def around(value, axes):
    total = None
    for axis in axes:
        count = value.shape[axis]
        both = pltpu.roll(value, 1, axis) + pltpu.roll(value, count - 1, axis)
        total = both if total is None else total + both
    return total


def coarse_kernel(*refs):
    blocks, (out, src, mid) = refs[:8], refs[8:]
    planes, half_y, half_z = blocks[0].shape
    at_y, at_z = lax.axis_index("gy"), lax.axis_index("gz")
    places = ((at_y, at_z), (1 - at_y, at_z), (at_y, 1 - at_z), (1 - at_y, 1 - at_z))
    for source, rim, (y, z) in zip(blocks[:4], blocks[4:], places):
        rows = pl.ds(pl.multiple_of(y * half_y, half_y), half_y)
        lanes = pl.ds(pl.multiple_of(z * half_z, half_z), half_z)
        src[:SWEEPS, rows, lanes] = rim[:SWEEPS]
        src[SWEEPS : SWEEPS + planes, rows, lanes] = source[...]
        src[SWEEPS + planes :, rows, lanes] = rim[SWEEPS:]
    inverse = 1.0 / (1.0 + 6.0 * coarse_coupling)
    total = src.shape[0]

    def relax(fields, plane):
        sides = fields[plane + 1] + fields[plane - 1] + around(fields[plane], (0, 1))
        return (src[plane] + coarse_coupling * sides) * inverse

    for plane in range(1, total - 1):
        mid[plane] = relax(src, plane)
    for plane in range(SWEEPS, total - SWEEPS):
        out[plane - SWEEPS] = relax(mid, plane)


def pairs_x():
    count = lax.axis_size("gx")
    even = [(i, i + 1 if i % 2 == 0 else i - 1) for i in range(count)]
    odd = [(i, (i + 1) % count if i % 2 else (i - 1) % count) for i in range(count)]
    return even, odd


def swap_x(first, second):
    even, odd = pairs_x()
    second = lax.ppermute(second, "gx", odd)
    first = lax.ppermute(first, "gx", even)
    return first, second


def swap(value, axis):
    return lax.ppermute(value, axis, [(0, 1), (1, 0)])


def swap_yz(band, side, corner):
    band = swap(band, "gy")
    corner = lax.ppermute(corner, ("gy", "gz"), [(0, 3), (3, 0), (1, 2), (2, 1)])
    side = swap(side, "gz")
    return band, side, corner


def gather_yz(value):
    along = swap(value, "gy")
    across = swap(value, "gz")
    diagonal = swap(along, "gz")
    return value, along, across, diagonal


def fused(fine_start, increments, coarse_start):
    depth, width, length = fine_start.shape
    half = (depth // 2, width // 2, length // 2)
    planes = (SWEEPS, width, length)
    padded = (3, width + 2 * CELLS, LANES)
    strips = ((SWEEPS + 1) * ROWS + SWEEPS * half[1] // 2, length)
    own = reaction(fine_start, increments[0], fine_step)
    even, odd = pairs_x()
    count = lax.axis_size("gx")
    rise = [(i, (i + 1) % count) for i in range(count)]
    fall = [(j, i) for i, j in rise]
    low = lax.ppermute(own[depth - SWEEPS :], "gx", rise)
    band, more, side, corner = call(
        halo_kernel,
        [(depth, ROWS, length), (depth // 2, ROWS, length), (2 * depth, width, LANES), (ROWS, LANES)],
        (own, increments),
    )
    halo_in = swap_yz(band, side, corner)
    more = swap(more, "gy")
    high = lax.ppermute(own[:SWEEPS], "gx", fall)
    (quarter,) = call(
        restrict_kernel,
        [half],
        (increments, coarse_start),
        scratch=[pltpu.VMEM((length // LANES, depth // 2, width, LANES), jnp.float32)],
    )
    first, second = call(strip_kernel, [strips, strips], (quarter,) + halo_in)
    strip_one, strip_two = swap_x(first, second)
    (forcing,) = call(scale_kernel, [fine_start.shape], (increments,))
    whole, later = call(
        spread_kernel,
        [(depth,) + padded, (depth,) + padded],
        (own, forcing, halo_in[0], more) + halo_in[1:],
    )
    quarters = gather_yz(quarter)
    mid, state = call(inner_kernel, [(depth - 2,) + padded, (depth - 4,) + padded], (whole, later))

    def outer(kernel, *halo):
        return call(
            kernel,
            [(SWEEPS,) + padded, planes],
            (whole, later, mid) + halo,
            scratch=[pltpu.VMEM((SWEEPS,) + padded, jnp.float32)] * 2,
        )

    edge_two, second = outer(first_outer, low, high, strip_two)
    add_two = lax.ppermute(second, "gx", odd)
    edge_one, first = outer(second_outer, low, high, strip_one)
    add_one = lax.ppermute(first, "gx", even)
    (column,) = call(column_kernel, [(2 * SWEEPS,) + half[1:]], (strip_one, strip_two))
    columns = gather_yz(column)
    hbm = pl.BlockSpec(memory_space=pltpu.HBM)
    vmem = pl.BlockSpec(memory_space=pltpu.VMEM)
    partial, rim = call(
        close_kernel,
        [fine_start.shape, (2 * SWEEPS, width, length)],
        (state, edge_one, edge_two),
        scratch=[
            pltpu.VMEM((depth,) + padded, jnp.float32),
            pltpu.VMEM((SWEEPS,) + padded, jnp.float32),
            pltpu.VMEM((SWEEPS,) + padded, jnp.float32),
            pltpu.VMEM((depth - 2 * SWEEPS, width, length), jnp.float32),
            pltpu.SemaphoreType.DMA((1,)),
        ],
        places=[hbm, vmem],
    )
    slab = pltpu.VMEM((half[0] + 2 * SWEEPS,) + coarse_start.shape[1:], jnp.float32)
    (coarse_final,) = call(
        coarse_kernel, [coarse_start.shape], quarters + columns, scratch=[slab, slab]
    )
    (fine_final,) = call(
        add_kernel,
        [fine_start.shape],
        (partial, rim, add_one, add_two),
        inputs=[hbm, vmem, vmem, vmem],
        places=[hbm],
        alias={0: 0},
        scratch=[pltpu.VMEM(planes, jnp.float32)] * 2 + [pltpu.SemaphoreType.DMA((2,))],
    )
    return (fine_final, coarse_final)


def body(fine_start, increments, coarse_start):
    depth, width, length = fine_start.shape
    fits = (
        lax.axis_size("gy") == 2
        and lax.axis_size("gz") == 2
        and lax.axis_size("gx") % 2 == 0
        and (STEPS, SWEEPS) == (2, 2)
        and depth >= 2 * REACH
        and depth % 2 == 0
        and (depth + depth // 2) * ROWS <= LANES
        and width % (4 * ROWS) == 0
        and width // ROWS + 1 <= LANES // ROWS
        and length == 2 * LANES
    )
    if not fits:
        return staged(fine_start, increments, coarse_start)
    return fused(fine_start, increments, coarse_start)


def solution(mesh):
    return jax.shard_map(
        body,
        mesh=mesh,
        in_specs=(
            P(("pairs", "gx"), "gy", "gz"),
            P(None, ("pairs", "gx"), "gy", "gz"),
            P(("pairs", "gx"), None, None),
        ),
        out_specs=(P(("pairs", "gx"), "gy", "gz"), P(("pairs", "gx"), None, None)),
        check_vma=False,
    )
```
